32 devices in a mesh: tm: 4 (over y, x), slab: 8 (over z, core).
Axes of the slice: x: 2, y: 2, z: 4, core: 2. Of those that a mesh axis runs over, the one named last changes fastest.
Arguments:
- velocity: bfloat16 [4, 3, 2, 131072], P('tm', None, None, 'slab'), may hold values from -64 to 64
- shell_index: int32 [131072], P('slab'), may hold values from 0 to 127, as said below
- ref_order: int32 [4], replicated, may hold values from 0 to 3, each once
Outputs:
- coherence: float32 [4, 4, 128], P('tm')
- spectrum: float32 [4, 128], P('tm')
The draws below stay inside these ranges and needn't reach their ends.
Inputs may be any that keep to these rules, and one draw needn't show every extreme that they name: `shell_index`: every shell number from 0 to 127 is taken by some mode. `ref_order`: each snapshot number appears once.
All inputs are finite; a program needn't handle non-finite values.
Results may differ from the reference program's by a relative error of at most 0.0003.
Values may be sent and summed in bfloat16 or wider, within the bound.
A program may use at most 64 MiB of HBM per device.

```python
import math
import jax
import jax.numpy as jnp
from jax import lax

SHELLS = 128
SNAPS = 4
MODES = 131072


def draw_velocity(key, part):
    keys = jax.random.split(jax.random.fold_in(key, 11), 5)
    amplitude = jnp.exp(jax.random.uniform(keys[0], (MODES,), jnp.float32, 0.0, math.log(10.0)))
    noise = jnp.clip(jax.random.normal(keys[1], (SNAPS, 3, 2, MODES), jnp.float32), -4.0, 4.0)
    persist = jax.random.uniform(keys[2], (MODES,), jnp.float32, 0.3, 0.97)
    scaling = jnp.exp(jax.random.uniform(keys[3], (SNAPS, 64), jnp.float32, math.log(0.5), math.log(2.0)))
    turning = jax.random.uniform(keys[4], (MODES,), jnp.float32, 0.2, 1.0)
    keep_share = jnp.sqrt(1.0 - persist * persist)

    def advance(state, fresh):
        new_state = persist * state + keep_share * fresh
        return (new_state, new_state)
    last_state, states = lax.scan(advance, noise[0], noise[1:])
    states = jnp.concatenate([noise[0][None], states], axis=0)
    steps_taken = jnp.arange(SNAPS, dtype=jnp.int32).astype(jnp.float32)
    phase = steps_taken[:, None] * turning[None, :]
    cosine = jnp.cos(phase)[:, None, :]
    sine = jnp.sin(phase)[:, None, :]
    real_old = states[:, :, 0]
    imag_old = states[:, :, 1]
    real_new = real_old * cosine - imag_old * sine
    imag_new = real_old * sine + imag_old * cosine
    states = jnp.stack([real_new, imag_new], axis=2)
    position = jnp.arange(MODES, dtype=jnp.int32)
    band = position * 64 // MODES
    band_scale = scaling[:, band]
    values = states * amplitude[None, None, None, :] * band_scale[:, None, None, :]
    return jnp.clip(values, -64.0, 64.0).astype(jnp.bfloat16)


def draw_shell_index(key, part):
    first_draw = jax.random.randint(jax.random.fold_in(key, 23), (MODES,), 0, SHELLS, dtype=jnp.int32)
    second_draw = jax.random.randint(jax.random.fold_in(key, 29), (MODES,), 0, SHELLS, dtype=jnp.int32)
    drawn = jnp.maximum(first_draw, second_draw)
    position = jnp.arange(MODES, dtype=jnp.int32)
    stride = MODES // SHELLS
    forced = position // stride % SHELLS
    return jnp.where(position % stride == 0, forced, drawn).astype(jnp.int32)


def setup_inputs(seed: int = 0) -> dict:
    streams_of = jax.random.split(jax.random.key(seed), 4)
    velocity = draw_velocity(jax.random.fold_in(streams_of[3], 71), 0)
    shell_index = draw_shell_index(jax.random.fold_in(streams_of[3], 71), 0)
    ref_order = jax.random.permutation(streams_of[2], SNAPS).astype(jnp.int32)
    return dict(velocity=velocity, shell_index=shell_index, ref_order=ref_order)


def reference(velocity, shell_index, ref_order):
    fields = velocity.astype(jnp.float32)
    rotated = jnp.stack([fields[:, :, 1], -fields[:, :, 0]], axis=2)
    energy = jnp.sum(fields * fields, axis=(1, 2)).astype(jnp.bfloat16)
    energy = lax.optimization_barrier(energy).astype(jnp.float32)
    spectrum = jax.ops.segment_sum(energy.T, shell_index, num_segments=SHELLS).T

    def one_snapshot(snapshot):
        own_field = lax.dynamic_index_in_dim(fields, snapshot, 0, keepdims=False)
        own_rotated = lax.dynamic_index_in_dim(rotated, snapshot, 0, keepdims=False)
        real_part = jnp.einsum("cpm,scpm->sm", own_field, fields, precision=lax.Precision.HIGHEST)
        imag_part = jnp.einsum("cpm,scpm->sm", own_rotated, fields, precision=lax.Precision.HIGHEST)
        stacked = jnp.stack([real_part, imag_part], axis=0).astype(jnp.bfloat16)
        stacked = lax.optimization_barrier(stacked).astype(jnp.float32)
        binned = jax.ops.segment_sum(stacked.reshape(2 * SNAPS, MODES).T, shell_index, num_segments=SHELLS)
        return binned.T.reshape(2, SNAPS, SHELLS)

    pair_sums = lax.map(one_snapshot, jnp.arange(SNAPS, dtype=jnp.int32))
    chosen = pair_sums[:, :, ref_order]
    power_sum = chosen[:, 0] * chosen[:, 0] + chosen[:, 1] * chosen[:, 1]
    coherence = power_sum / (spectrum[:, None, :] * spectrum[ref_order][None, :, :])
    return coherence, spectrum
```

```python
import functools

import jax
import jax.numpy as jnp
from jax import lax
from jax.experimental import pallas as pl
from jax.experimental.pallas import tpu as pltpu
from jax.sharding import PartitionSpec as P

SHELLS = 128
LANES = 128
CORES = 2
HUB = 1
CHUNKS = 2
MESH = pl.DeviceIdType.MESH


def kernel(
    snaps, slabs, rows, direct,
    vel_ref, ids_ref, order_ref,
    coh_ref, spec_ref,
    staged, ids, order, got, split, terms, lhs, hot, mine, packs, near, mid, far, rest, total, ready,
    load_sem, stage_sem, ids_send, ids_recv, send_sem, recv_sem, near_send, near_recv,
    far_send, far_recv, rest_send, rest_recv,
):
    tm = lax.axis_index("tm")
    slab = lax.axis_index("slab")
    core = lax.rem(slab, CORES)
    place = lax.div(slab, CORES)
    places = slabs // CORES
    pairs = snaps * snaps
    part = rows // CHUNKS
    hub = core == HUB
    leaf = core != HUB
    root = jnp.logical_and(tm == 0, place == 0)
    outer = place != 0

    others = []
    for high in reversed(range(snaps // 2)):
        for low in (1, 0):
            other_high = lax.rem(lax.div(tm, 2) + high, snaps // 2)
            others.append(other_high * 2 + lax.rem(lax.rem(tm, 2) + low, 2))
    others = others[:-1]
    aways = [lax.rem(place + offset, places) for offset in range(1, places)]

    def hub_of(snap, where):
        return (snap, where * CORES + HUB)

    def leaf_of(snap, where):
        return (snap, where * CORES + 1 - HUB)

    barrier = pltpu.get_barrier_semaphore()

    def tell(device):
        pl.semaphore_signal(barrier, inc=1, device_id=device, device_id_type=MESH)

    def share_of(snap):
        return pl.ds(pl.multiple_of(snap * 2 * rows, 2 * rows), 2 * rows)

    def send(src, dst, send_to, recv_at, device):
        pltpu.make_async_remote_copy(
            src_ref=src, dst_ref=dst, send_sem=send_to, recv_sem=recv_at,
            device_id=device, device_id_type=MESH,
        ).start()

    def drain(ref, sem):
        pltpu.make_async_copy(ref, ref, sem).wait()

    for away in aways:
        tell(hub_of(tm, away))

    @pl.when(hub)
    def _():
        for other in others:
            tell(hub_of(other, place))
            tell(leaf_of(other, place))
        tell(leaf_of(tm, place))

    @pl.when(leaf)
    def _():
        tell(hub_of(tm, place))

    if direct:
        @pl.when(root)
        def _():
            for snap in range(1, snaps):
                for where in range(1, places):
                    tell(hub_of(snap, where))

    load_ids = pltpu.make_async_copy(
        ids_ref.at[pl.ds(pl.multiple_of(tm * rows, rows), rows)], ids.at[HUB], load_sem.at[1]
    )
    load_order = pltpu.make_async_copy(order_ref, order, load_sem.at[2])
    for other in others:
        pltpu.make_async_copy(vel_ref.at[:, share_of(other)], staged.at[other], stage_sem).start()
    load_ids.start()

    def exchange(peers):
        for h in range(CHUNKS):
            for peer in peers:
                send(
                    staged.at[peer, :, pl.ds(h * 2 * part, 2 * part)], got.at[core, h, tm],
                    send_sem, recv_sem.at[core * CHUNKS + h], hub_of(peer, place),
                )

    @pl.when(leaf)
    def _():
        pltpu.make_async_copy(vel_ref.at[:, share_of(tm)], staged.at[tm], stage_sem).start()
        load_order.start()
        pl.semaphore_wait(barrier, snaps)
        drain(staged, stage_sem)
        exchange(others + [tm])
        load_ids.wait()
        send(ids.at[HUB], ids.at[1 - HUB], ids_send, ids_recv, hub_of(tm, place))

    @pl.when(hub)
    def _():
        for h in range(CHUNKS):
            pltpu.make_async_copy(
                vel_ref.at[:, pl.ds(pl.multiple_of((tm * CHUNKS + h) * 2 * part, 2 * part), 2 * part)],
                got.at[HUB, h, tm], load_sem.at[0],
            ).start()
        load_order.start()
        heard = (snaps - 1) + (places - 1) + places
        if direct:
            heard = heard + jnp.where(jnp.logical_and(tm != 0, outer), CORES, 0)
        pl.semaphore_wait(barrier, heard)
        drain(staged.at[pl.ds(0, snaps - 1)], stage_sem)
        exchange(others)

        load_ids.wait()
        shell = lax.broadcasted_iota(jnp.int32, (SHELLS, LANES), 0)

        def one_hot(unit):
            for j in range(rows):
                same = shell == jnp.broadcast_to(ids[unit, j : j + 1, :], (SHELLS, LANES))
                hot[unit, :, j * LANES : (j + 1) * LANES] = jnp.where(same, 1.0, 0.0).astype(jnp.bfloat16)

        one_hot(HUB)
        drain(ids.at[1 - HUB], ids_recv)
        one_hot(1 - HUB)
        drain(got.at[HUB, :, 0], load_sem.at[0])

        def work(unit, h, first):
            count = snaps - 1 if unit == HUB else snaps
            drain(got.at[unit, h, pl.ds(0, count)], recv_sem.at[unit * CHUNKS + h])
            real, imag = {}, {}
            for t in range(snaps):
                for c in range(3):
                    split[t * 3 + c] = got[unit, h, t, c].astype(jnp.float32)
            for t in range(snaps):
                for c in range(3):
                    real[t, c] = split[t * 3 + c, pl.ds(0, part, stride=2), :]
                    imag[t, c] = split[t * 3 + c, pl.ds(1, part, stride=2), :]
            for t in range(snaps):
                for r in range(t, snaps):
                    value = real[t, 0] * real[r, 0] + imag[t, 0] * imag[r, 0]
                    for c in (1, 2):
                        value = value + real[t, c] * real[r, c]
                        value = value + imag[t, c] * imag[r, c]
                    terms[(t * snaps + r) * part : (t * snaps + r + 1) * part] = value
                    if r > t:
                        value = imag[t, 0] * real[r, 0] - real[t, 0] * imag[r, 0]
                        for c in (1, 2):
                            value = value + imag[t, c] * real[r, c]
                            value = value - real[t, c] * imag[r, c]
                        terms[(r * snaps + t) * part : (r * snaps + t + 1) * part] = value
            for j in range(part):
                block = terms[pl.ds(j, pairs, stride=part), :]
                lhs[:, j * LANES : (j + 1) * LANES] = block.astype(jnp.bfloat16)
            value = lax.dot_general(
                lhs[...], hot[unit, :, h * part * LANES : (h + 1) * part * LANES],
                (((1,), (1,)), ((), ())), preferred_element_type=jnp.float32,
            )
            mine[...] = value if first else mine[...] + value

        first = True
        for h in range(CHUNKS):
            for unit in (HUB, 1 - HUB):
                work(unit, h, first)
                first = False

        diagonal = mine[pl.ds(0, snaps, stride=snaps + 1), :]
        for t in range(snaps):
            packs[t, :snaps] = mine[t * snaps : (t + 1) * snaps, :]
            packs[t, snaps : 2 * snaps] = mine[pl.ds(t, snaps, stride=snaps), :]
            packs[t, 2 * snaps :] = diagonal
        for other in others:
            send(packs.at[other], near.at[tm], near_send, near_recv, hub_of(other, place))
        if direct:
            @pl.when(outer)
            def _():
                slot = (place - 1) * snaps + tm
                send(packs.at[0], rest.at[slot], rest_send, rest_recv, leaf_of(0, 0))
                send(packs.at[0], rest.at[slot], rest_send, rest_recv, hub_of(0, 0))
        near[tm] = packs[tm]
        drain(near.at[pl.ds(0, snaps - 1)], near_recv)
        value = near[0]
        for t in range(1, snaps):
            value = value + near[t]
        mid[...] = value

        for away in aways:
            if direct:
                @pl.when(jnp.logical_or(tm != 0, away != 0))
                def _():
                    send(mid, far.at[place], far_send, far_recv, leaf_of(tm, away))
                    send(mid, far.at[place], far_send, far_recv, hub_of(tm, away))
            else:
                send(mid, far.at[place], far_send, far_recv, leaf_of(tm, away))
                send(mid, far.at[place], far_send, far_recv, hub_of(tm, away))
        send(mid, far.at[place], far_send, far_recv, leaf_of(tm, place))
        far[place] = mid[...]

    def gather():
        @pl.when(hub)
        def _():
            drain(far.at[pl.ds(0, places - 1)], far_recv)

        @pl.when(leaf)
        def _():
            drain(far.at[pl.ds(0, places)], far_recv)

        value = far[0]
        for where in range(1, places):
            value = value + far[where]
        total[...] = value

    if direct:
        @pl.when(root)
        def _():
            @pl.when(leaf)
            def _():
                drain(far.at[0], far_recv)

            drain(rest, rest_recv)
            value = far[0]
            for where in range(places - 1):
                share = rest[where * snaps]
                for t in range(1, snaps):
                    share = share + rest[where * snaps + t]
                value = value + share
            total[...] = value

        pl.when(jnp.logical_not(root))(gather)
    else:
        gather()

    load_order.wait()
    across = total[:snaps]
    down = total[snaps : 2 * snaps]
    spectra = total[2 * snaps :]
    own_spectrum = total[pl.ds(2 * snaps + tm, 1), :]
    which = lax.broadcasted_iota(jnp.int32, (snaps, SHELLS), 0)
    down = jnp.where(which == tm, 0.0, down)
    ready[...] = (across * across + down * down) / (own_spectrum * spectra)
    for j in range(snaps):
        coh_ref[0, j : j + 1, :] = ready[pl.ds(order[j], 1), :]
    spec_ref[...] = own_spectrum

    @pl.when(leaf)
    def _():
        drain(staged, send_sem)
        drain(ids.at[HUB], ids_send)

    @pl.when(hub)
    def _():
        drain(staged.at[pl.ds(0, snaps - 1)], send_sem)
        drain(near.at[pl.ds(0, snaps - 1)], near_send)
        if direct:
            short = jnp.logical_and(tm == 0, outer)

            @pl.when(short)
            def _():
                drain(far.at[pl.ds(0, 2 * places - 3)], far_send)

            @pl.when(jnp.logical_not(short))
            def _():
                drain(far.at[pl.ds(0, 2 * places - 1)], far_send)

            @pl.when(outer)
            def _():
                drain(rest.at[pl.ds(0, CORES)], rest_send)
        else:
            drain(far.at[pl.ds(0, 2 * places - 1)], far_send)


def put(coh_ref, spec_ref, coh_out, spec_out, sems):
    copies = [
        pltpu.make_async_copy(coh_ref, coh_out, sems.at[0]),
        pltpu.make_async_copy(spec_ref, spec_out, sems.at[1]),
    ]
    for copy in copies:
        copy.start()
    for copy in copies:
        copy.wait()


def body(velocity, shell_index, ref_order):
    snaps = lax.axis_size("tm")
    slabs = lax.axis_size("slab")
    places = slabs // CORES
    modes = velocity.shape[3]
    blocks = modes // LANES
    rows = blocks // snaps
    part = rows // CHUNKS
    pairs = snaps * snaps
    high = 3 * snaps
    direct = places * snaps <= 32 and places > 1
    vel = velocity.reshape(3, 2, blocks, LANES).transpose(0, 2, 1, 3)
    vel = vel.reshape(3, 2 * blocks, LANES)
    ids = shell_index.reshape(blocks, LANES)
    coherence, spectrum = pl.pallas_call(
        functools.partial(kernel, snaps, slabs, rows, direct),
        out_shape=(
            pltpu.VMEM((1, snaps, SHELLS), jnp.float32),
            pltpu.VMEM((1, SHELLS), jnp.float32),
        ),
        in_specs=[
            pl.BlockSpec(memory_space=pl.ANY),
            pl.BlockSpec(memory_space=pl.ANY),
            pl.BlockSpec(memory_space=pl.ANY),
        ],
        out_specs=(
            pl.BlockSpec(memory_space=pltpu.VMEM),
            pl.BlockSpec(memory_space=pltpu.VMEM),
        ),
        scratch_shapes=[
            pltpu.VMEM((snaps, 3, 2 * rows, LANES), jnp.bfloat16),
            pltpu.VMEM((CORES, rows, LANES), jnp.int32),
            pltpu.SMEM((snaps,), jnp.int32),
            pltpu.VMEM((CORES, CHUNKS, snaps, 3, 2 * part, LANES), jnp.bfloat16),
            pltpu.VMEM((snaps * 3, 2 * part, LANES), jnp.float32),
            pltpu.VMEM((pairs * part, LANES), jnp.float32),
            pltpu.VMEM((pairs, part * LANES), jnp.bfloat16),
            pltpu.VMEM((CORES, SHELLS, rows * LANES), jnp.bfloat16),
            pltpu.VMEM((pairs, SHELLS), jnp.float32),
            pltpu.VMEM((snaps, high, SHELLS), jnp.float32),
            pltpu.VMEM((snaps, high, SHELLS), jnp.float32),
            pltpu.VMEM((high, SHELLS), jnp.float32),
            pltpu.VMEM((2 * places, high, SHELLS), jnp.float32),
            pltpu.VMEM(((places - 1) * snaps if direct else 1, high, SHELLS), jnp.float32),
            pltpu.VMEM((high, SHELLS), jnp.float32),
            pltpu.VMEM((snaps, SHELLS), jnp.float32),
            pltpu.SemaphoreType.DMA((3,)),
            pltpu.SemaphoreType.DMA,
            pltpu.SemaphoreType.DMA,
            pltpu.SemaphoreType.DMA,
            pltpu.SemaphoreType.DMA,
            pltpu.SemaphoreType.DMA((CORES * CHUNKS,)),
            pltpu.SemaphoreType.DMA,
            pltpu.SemaphoreType.DMA,
            pltpu.SemaphoreType.DMA,
            pltpu.SemaphoreType.DMA,
            pltpu.SemaphoreType.DMA,
            pltpu.SemaphoreType.DMA,
        ],
        compiler_params=pltpu.CompilerParams(collective_id=0, has_side_effects=True),
    )(vel, ids, ref_order)
    coherence = pltpu.with_memory_space_constraint(coherence, pltpu.VMEM)
    spectrum = pltpu.with_memory_space_constraint(spectrum, pltpu.VMEM)
    return pl.pallas_call(
        put,
        out_shape=(
            jax.ShapeDtypeStruct((1, snaps, SHELLS), jnp.float32),
            jax.ShapeDtypeStruct((1, SHELLS), jnp.float32),
        ),
        in_specs=[pl.BlockSpec(memory_space=pltpu.VMEM)] * 2,
        out_specs=(pl.BlockSpec(memory_space=pl.ANY),) * 2,
        scratch_shapes=[pltpu.SemaphoreType.DMA((2,))],
    )(coherence, spectrum)


def solution(mesh):
    in_specs = (P("tm", None, None, "slab"), P("slab"), P())
    out_specs = (P("tm", None, None), P("tm", None))
    return jax.shard_map(body, mesh=mesh, in_specs=in_specs, out_specs=out_specs, check_vma=False)
```

```python
import functools

import jax
import jax.numpy as jnp
from jax import lax
from jax.experimental import pallas as pl
from jax.experimental.pallas import tpu as pltpu
from jax.sharding import PartitionSpec as P

SHELLS = 128
LANES = 128
CORES = 2
HUB = 1
PART = 8
MESH = pl.DeviceIdType.MESH


def plan(rows):
    base = rows // PART
    skew = 1 if base >= 3 else 0
    low = base - skew
    slots = [(0, low - 1, 0)] if low > 1 else []
    slots += [(low - 1 + extra, 1, extra + 1) for extra in range(2 * skew)]
    slots.append((low - 1 + 2 * skew, 1, 0))
    return base, skew, low, slots


def kernel(
    snaps, slabs, rows,
    vel_ref, ids_ref, order_ref,
    coh_ref, spec_ref,
    staged, ids, order, got, split, terms, lhs, hot, mine, packs, inbox, total, ready,
    load_sem, stage_sem, ids_send, ids_recv, send_sem, recv_sem, pack_send, pack_recv,
    near_ok, far_ok,
):
    tm = lax.axis_index("tm")
    slab = lax.axis_index("slab")
    core = lax.rem(slab, CORES)
    place = lax.div(slab, CORES)
    places = slabs // CORES
    pairs = snaps * snaps
    blocks = rows * snaps
    base, skew, low, slots = plan(rows)
    hub = core == HUB
    leaf = core != HUB
    me = place * snaps + tm
    last = snaps - 1
    gate = tm == last

    others = []
    for high in reversed(range(snaps // 2)):
        for low_bit in (1, 0):
            other_high = lax.rem(lax.div(tm, 2) + high, snaps // 2)
            others.append(other_high * 2 + lax.rem(lax.rem(tm, 2) + low_bit, 2))
    others = others[:-1]
    aways = [lax.rem(place + offset, places) for offset in range(1, places)]

    def hub_of(snap, where):
        return (snap, where * CORES + HUB)

    def leaf_of(snap, where):
        return (snap, where * CORES + 1 - HUB)

    def count_of(snap):
        return base + jnp.where(snap == 0, skew, 0) - jnp.where(snap == last, skew, 0)

    def source_of(snap, slot):
        first = snap * base
        if skew:
            first = first + jnp.where(snap == 0, 0, skew)
        at = slots[slot][0]
        if slot == len(slots) - 1:
            at = count_of(snap) - 1
        return first + at

    def piece(start, units, scale):
        size = PART * scale
        return pl.ds(pl.multiple_of(start * size, size), units * size)

    barrier = pltpu.get_barrier_semaphore()

    def tell(device):
        pl.semaphore_signal(barrier, inc=1, device_id=device, device_id_type=MESH)

    def send(src, dst, send_to, recv_at, device):
        pltpu.make_async_remote_copy(
            src_ref=src, dst_ref=dst, send_sem=send_to, recv_sem=recv_at,
            device_id=device, device_id_type=MESH,
        ).start()

    def drain(ref, sem):
        pltpu.make_async_copy(ref, ref, sem).wait()

    def for_slots(snap, run):
        for slot, (_, _, need) in enumerate(slots):
            if need:
                pl.when(count_of(snap) >= low + need)(functools.partial(run, slot))
            else:
                run(slot)

    load_order = pltpu.make_async_copy(order_ref, order, load_sem.at[2])
    for part in range(snaps):
        span = pl.ds(part * 2 * rows, 2 * rows)
        pltpu.make_async_copy(vel_ref.at[:, span], staged.at[:, span], stage_sem).start()

    @pl.when(leaf)
    def _():
        @pl.when(gate)
        def _():
            tell(hub_of(tm, place))

        @pl.when(jnp.logical_not(gate))
        def _():
            tell(leaf_of(last, place))

    @pl.when(hub)
    def _():
        for other in others:
            tell(hub_of(other, place))
        for snap in range(last):
            tell(leaf_of(snap, place))

    for away in aways:
        tell(leaf_of(last, away))

    load_order.start()

    def load_ids(slot):
        at, units, _ = slots[slot]
        pltpu.make_async_copy(
            ids_ref.at[piece(source_of(tm, slot), units, 1)],
            ids.at[HUB, pl.ds(at * PART, units * PART)], load_sem.at[1],
        ).start()

    for_slots(tm, load_ids)

    def drain_ids(ref, sem):
        for units in range(low, low + 2 * skew + 1):
            @pl.when(count_of(tm) == units)
            def _():
                drain(ref.at[pl.ds(0, units * PART)], sem)

    def exchange(peers):
        for slot in range(len(slots)):
            for peer in peers:
                at, units, need = slots[slot]

                def ship(peer=peer, slot=slot, at=at, units=units):
                    send(
                        staged.at[:, piece(source_of(peer, slot), units, 2)],
                        got.at[core, tm, :, pl.ds(at * 2 * PART, units * 2 * PART)],
                        send_sem, recv_sem.at[core * len(slots) + slot], hub_of(peer, place),
                    )

                if need:
                    pl.when(count_of(peer) >= low + need)(ship)
                else:
                    ship()

    @pl.when(leaf)
    def _():
        drain_ids(ids.at[HUB], load_sem.at[1])

        @pl.when(gate)
        def _():
            pl.semaphore_wait(near_ok, 1)

        @pl.when(jnp.logical_not(gate))
        def _():
            pl.semaphore_wait(barrier, snaps)

        drain(staged, stage_sem)

        def ship_ids(slot):
            at, units, _ = slots[slot]
            span = pl.ds(at * PART, units * PART)
            send(ids.at[HUB, span], ids.at[1 - HUB, span], ids_send, ids_recv, hub_of(tm, place))

        for_slots(tm, ship_ids)
        exchange(others + [tm])

        @pl.when(gate)
        def _():
            pl.semaphore_wait(barrier, last + CORES * snaps * (places - 1))
            for snap in range(snaps):
                pl.semaphore_signal(
                    far_ok, inc=1, device_id=hub_of(snap, place), device_id_type=MESH
                )

    @pl.when(hub)
    def _():
        def load_own(slot):
            at, units, _ = slots[slot]
            pltpu.make_async_copy(
                vel_ref.at[:, piece(source_of(tm, slot), units, 2)],
                got.at[HUB, tm, :, pl.ds(at * 2 * PART, units * 2 * PART)], load_sem.at[0],
            ).start()

        for_slots(tm, load_own)
        pl.semaphore_wait(barrier, last + jnp.where(gate, 1, 0))

        @pl.when(gate)
        def _():
            pl.semaphore_signal(
                near_ok, inc=1, device_id=leaf_of(tm, place), device_id_type=MESH
            )

        drain(staged, stage_sem)
        exchange(others)
        mine[...] = jnp.zeros_like(mine)
        shell = lax.broadcasted_iota(jnp.int32, (SHELLS, LANES), 0)

        def one_hot(unit, slot):
            at, units, _ = slots[slot]
            for j in range(at * PART, (at + units) * PART):
                same = shell == jnp.broadcast_to(ids[unit, j : j + 1, :], (SHELLS, LANES))
                hot[unit, :, j * LANES : (j + 1) * LANES] = jnp.where(same, 1.0, 0.0).astype(jnp.bfloat16)

        drain_ids(ids.at[HUB], load_sem.at[1])
        for_slots(tm, functools.partial(one_hot, HUB))
        drain_ids(ids.at[1 - HUB], ids_recv)
        for_slots(tm, functools.partial(one_hot, 1 - HUB))
        for units in range(low, low + 2 * skew + 1):
            @pl.when(count_of(tm) == units)
            def _():
                drain(got.at[HUB, 0, :, pl.ds(0, units * 2 * PART)], load_sem.at[0])

        def prepare(unit, at, row):
            span = pl.ds(at * 2 * PART, 2 * PART)
            real, imag = {}, {}
            for t in range(snaps):
                for c in range(3):
                    split[row, t * 3 + c] = got[unit, t, c, span, :].astype(jnp.float32)
            for t in range(snaps):
                for c in range(3):
                    real[t, c] = split[row, t * 3 + c, pl.ds(0, PART, stride=2), :]
                    imag[t, c] = split[row, t * 3 + c, pl.ds(1, PART, stride=2), :]
            for t in range(snaps):
                for r in range(t, snaps):
                    value = real[t, 0] * real[r, 0] + imag[t, 0] * imag[r, 0]
                    for c in (1, 2):
                        value = value + real[t, c] * real[r, c]
                        value = value + imag[t, c] * imag[r, c]
                    terms[row, (t * snaps + r) * PART : (t * snaps + r + 1) * PART] = value
                    if r > t:
                        value = imag[t, 0] * real[r, 0] - real[t, 0] * imag[r, 0]
                        for c in (1, 2):
                            value = value + imag[t, c] * real[r, c]
                            value = value - real[t, c] * imag[r, c]
                        terms[row, (r * snaps + t) * PART : (r * snaps + t + 1) * PART] = value
            for j in range(PART):
                block = terms[row, pl.ds(j, pairs, stride=PART), :]
                lhs[row, :, j * LANES : (j + 1) * LANES] = block.astype(jnp.bfloat16)

        wide = PART * LANES // 2

        def work(slot):
            at, units, _ = slots[slot]
            span = pl.ds(at * 2 * PART, units * 2 * PART)
            jobs = []
            for unit in (HUB, 1 - HUB):
                senders = snaps - 1 if unit == HUB else snaps
                drain(got.at[unit, pl.ds(0, senders), :, span], recv_sem.at[unit * len(slots) + slot])
                for step in range(units):
                    row = len(jobs)
                    prepare(unit, at + step, row)
                    jobs.append((unit, at + step, row))
            for side in range(2):
                value = mine[side]
                for unit, spot, row in jobs:
                    start = spot * PART * LANES + side * wide
                    value = value + lax.dot_general(
                        lhs[row, :, side * wide : (side + 1) * wide], hot[unit, :, start : start + wide],
                        (((1,), (1,)), ((), ())), preferred_element_type=jnp.float32,
                    )
                mine[side] = value

        for_slots(tm, work)

        def row_of(index):
            return mine[0, index, :] + mine[1, index, :]

        diagonal = row_of(pl.ds(0, snaps, stride=snaps + 1))
        for t in range(snaps):
            packs[t, :snaps] = row_of(pl.ds(t * snaps, snaps))
            packs[t, snaps : 2 * snaps] = row_of(pl.ds(t, snaps, stride=snaps))
            packs[t, 2 * snaps :] = diagonal
        pl.semaphore_wait(far_ok, 1)
        for where in range(places):
            for snap in range(snaps):
                send(packs.at[snap], inbox.at[me], pack_send, pack_recv, leaf_of(snap, where))

                @pl.when(me != where * snaps + snap)
                def _():
                    send(packs.at[snap], inbox.at[me], pack_send, pack_recv, hub_of(snap, where))
        inbox[me] = packs[tm]
        drain(inbox.at[pl.ds(0, snaps * places - 1)], pack_recv)

    @pl.when(leaf)
    def _():
        drain(inbox.at[pl.ds(0, snaps * places)], pack_recv)

    value = inbox[0]
    for n in range(1, snaps * places):
        value = value + inbox[n]
    total[...] = value

    load_order.wait()
    across = total[:snaps]
    down = total[snaps : 2 * snaps]
    spectra = total[2 * snaps :]
    own_spectrum = total[pl.ds(2 * snaps + tm, 1), :]
    which = lax.broadcasted_iota(jnp.int32, (snaps, SHELLS), 0)
    down = jnp.where(which == tm, 0.0, down)
    ready[...] = (across * across + down * down) / (own_spectrum * spectra)
    for j in range(snaps):
        coh_ref[0, j : j + 1, :] = ready[pl.ds(order[j], 1), :]
    spec_ref[...] = own_spectrum

    @pl.when(leaf)
    def _():
        drain(staged, send_sem)
        drain_ids(ids.at[HUB], ids_send)

    @pl.when(hub)
    def _():
        for units in range(low, low + 2 * skew + 1):
            @pl.when(count_of(tm) == units)
            def _():
                drain(staged.at[:, pl.ds(0, 2 * (blocks - units * PART))], send_sem)
        drain(inbox.at[pl.ds(0, 2 * snaps * places - 1)], pack_send)


def put(coh_ref, spec_ref, coh_out, spec_out, sems):
    copies = [
        pltpu.make_async_copy(coh_ref, coh_out, sems.at[0]),
        pltpu.make_async_copy(spec_ref, spec_out, sems.at[1]),
    ]
    for copy in copies:
        copy.start()
    for copy in copies:
        copy.wait()


def body(velocity, shell_index, ref_order):
    snaps = lax.axis_size("tm")
    slabs = lax.axis_size("slab")
    places = slabs // CORES
    modes = velocity.shape[3]
    blocks = modes // LANES
    rows = blocks // snaps
    _, skew, low, slots = plan(rows)
    most = slots[-1][0] + 1
    jobs = CORES * max(units for _, units, _ in slots)
    pairs = snaps * snaps
    high = 3 * snaps
    vel = velocity.reshape(3, 2, blocks, LANES).transpose(0, 2, 1, 3)
    vel = vel.reshape(3, 2 * blocks, LANES)
    ids = shell_index.reshape(blocks, LANES)
    coherence, spectrum = pl.pallas_call(
        functools.partial(kernel, snaps, slabs, rows),
        out_shape=(
            pltpu.VMEM((1, snaps, SHELLS), jnp.float32),
            pltpu.VMEM((1, SHELLS), jnp.float32),
        ),
        in_specs=[
            pl.BlockSpec(memory_space=pl.ANY),
            pl.BlockSpec(memory_space=pl.ANY),
            pl.BlockSpec(memory_space=pl.ANY),
        ],
        out_specs=(
            pl.BlockSpec(memory_space=pltpu.VMEM),
            pl.BlockSpec(memory_space=pltpu.VMEM),
        ),
        scratch_shapes=[
            pltpu.VMEM((3, 2 * blocks, LANES), jnp.bfloat16),
            pltpu.VMEM((CORES, most * PART, LANES), jnp.int32),
            pltpu.SMEM((snaps,), jnp.int32),
            pltpu.VMEM((CORES, snaps, 3, most * 2 * PART, LANES), jnp.bfloat16),
            pltpu.VMEM((jobs, snaps * 3, 2 * PART, LANES), jnp.float32),
            pltpu.VMEM((jobs, pairs * PART, LANES), jnp.float32),
            pltpu.VMEM((jobs, pairs, PART * LANES), jnp.bfloat16),
            pltpu.VMEM((CORES, SHELLS, most * PART * LANES), jnp.bfloat16),
            pltpu.VMEM((2, pairs, SHELLS), jnp.float32),
            pltpu.VMEM((snaps, high, SHELLS), jnp.float32),
            pltpu.VMEM((2 * snaps * places, high, SHELLS), jnp.float32),
            pltpu.VMEM((high, SHELLS), jnp.float32),
            pltpu.VMEM((snaps, SHELLS), jnp.float32),
            pltpu.SemaphoreType.DMA((3,)),
            pltpu.SemaphoreType.DMA,
            pltpu.SemaphoreType.DMA,
            pltpu.SemaphoreType.DMA,
            pltpu.SemaphoreType.DMA,
            pltpu.SemaphoreType.DMA((CORES * len(slots),)),
            pltpu.SemaphoreType.DMA,
            pltpu.SemaphoreType.DMA,
            pltpu.SemaphoreType.REGULAR,
            pltpu.SemaphoreType.REGULAR,
        ],
        compiler_params=pltpu.CompilerParams(collective_id=0, has_side_effects=True),
    )(vel, ids, ref_order)
    coherence = pltpu.with_memory_space_constraint(coherence, pltpu.VMEM)
    spectrum = pltpu.with_memory_space_constraint(spectrum, pltpu.VMEM)
    return pl.pallas_call(
        put,
        out_shape=(
            jax.ShapeDtypeStruct((1, snaps, SHELLS), jnp.float32),
            jax.ShapeDtypeStruct((1, SHELLS), jnp.float32),
        ),
        in_specs=[pl.BlockSpec(memory_space=pltpu.VMEM)] * 2,
        out_specs=(pl.BlockSpec(memory_space=pl.ANY),) * 2,
        scratch_shapes=[pltpu.SemaphoreType.DMA((2,))],
    )(coherence, spectrum)


def solution(mesh):
    in_specs = (P("tm", None, None, "slab"), P("slab"), P())
    out_specs = (P("tm", None, None), P("tm", None))
    return jax.shard_map(body, mesh=mesh, in_specs=in_specs, out_specs=out_specs, check_vma=False)
```

```python
import functools

import jax
import jax.numpy as jnp
from jax import lax
from jax.experimental import pallas as pl
from jax.experimental.pallas import tpu as pltpu
from jax.sharding import PartitionSpec as P

SHELLS = 128
LANES = 128
CORES = 2
HUB = 1
PART = 8
MESH = pl.DeviceIdType.MESH


def plan(rows):
    base = rows // PART
    skew = 1 if base >= 3 else 0
    low = base - skew
    slots = [(0, low - 1, 0)] if low > 1 else []
    slots += [(low - 1 + extra, 1, extra + 1) for extra in range(2 * skew)]
    slots.append((low - 1 + 2 * skew, 1, 0))
    return base, skew, low, slots


def kernel(
    snaps, slabs, rows,
    vel_ref, ids_ref, order_ref,
    coh_ref, spec_ref,
    staged, ids, order, got, split, terms, lhs, hot, mine, packs, inbox, total, ready,
    load_sem, stage_sem, ids_send, ids_recv, send_sem, recv_sem, pack_send, pack_recv,
    near_ok, far_ok, late_ok,
):
    tm = lax.axis_index("tm")
    slab = lax.axis_index("slab")
    core = lax.rem(slab, CORES)
    place = lax.div(slab, CORES)
    places = slabs // CORES
    pairs = snaps * snaps
    blocks = rows * snaps
    base, skew, low, slots = plan(rows)
    hub = core == HUB
    leaf = core != HUB
    me = place * snaps + tm
    last = snaps - 1
    gate = tm == last
    head = tm == 0

    others = []
    for high in reversed(range(snaps // 2)):
        for low_bit in (1, 0):
            other_high = lax.rem(lax.div(tm, 2) + high, snaps // 2)
            others.append(other_high * 2 + lax.rem(lax.rem(tm, 2) + low_bit, 2))
    others = others[:-1]
    aways = [lax.rem(place + offset, places) for offset in range(1, places)]

    def hub_of(snap, where):
        return (snap, where * CORES + HUB)

    def leaf_of(snap, where):
        return (snap, where * CORES + 1 - HUB)

    def count_of(snap):
        if isinstance(snap, int):
            return base + (skew if snap == 0 else 0) - (skew if snap == last else 0)
        return base + jnp.where(snap == 0, skew, 0) - jnp.where(snap == last, skew, 0)

    def source_of(snap, slot):
        first = snap * base
        if skew:
            first = first + (jnp.where(snap == 0, 0, skew) if not isinstance(snap, int) else (skew if snap else 0))
        at = slots[slot][0]
        if slot == len(slots) - 1:
            at = count_of(snap) - 1
        return first + at

    def piece(start, units, scale):
        size = PART * scale
        if isinstance(start, int):
            return pl.ds(start * size, units * size)
        return pl.ds(pl.multiple_of(start * size, size), units * size)

    barrier = pltpu.get_barrier_semaphore()

    def tell(device):
        pl.semaphore_signal(barrier, inc=1, device_id=device, device_id_type=MESH)

    def send(src, dst, send_to, recv_at, device):
        pltpu.make_async_remote_copy(
            src_ref=src, dst_ref=dst, send_sem=send_to, recv_sem=recv_at,
            device_id=device, device_id_type=MESH,
        ).start()

    def drain(ref, sem):
        pltpu.make_async_copy(ref, ref, sem).wait()

    def for_slots(snap, run):
        for slot, (_, _, need) in enumerate(slots):
            if need:
                pl.when(count_of(snap) >= low + need)(functools.partial(run, slot))
            else:
                run(slot)

    load_order = pltpu.make_async_copy(order_ref, order, load_sem.at[2])
    for part in range(snaps):
        span = pl.ds(part * 2 * rows, 2 * rows)
        pltpu.make_async_copy(vel_ref.at[:, span], staged.at[:, span], stage_sem).start()

    @pl.when(leaf)
    def _():
        @pl.when(gate)
        def _():
            tell(hub_of(tm, place))

        @pl.when(jnp.logical_not(gate))
        def _():
            tell(leaf_of(last, place))

        @pl.when(head)
        def _():
            tell(hub_of(tm, place))

    @pl.when(hub)
    def _():
        @pl.when(gate)
        def _():
            tell(leaf_of(0, place))
            for snap in range(1, last):
                tell(hub_of(snap, place))

        @pl.when(jnp.logical_not(gate))
        def _():
            for snap in range(snaps):
                @pl.when(tm != snap)
                def _():
                    tell(hub_of(snap, place))

        for snap in range(1, last):
            tell(leaf_of(snap, place))

    for away in aways:
        tell(leaf_of(last, away))

    load_order.start()

    def load_ids(slot):
        at, units, _ = slots[slot]
        pltpu.make_async_copy(
            ids_ref.at[piece(source_of(tm, slot), units, 1)],
            ids.at[HUB, pl.ds(at * PART, units * PART)], load_sem.at[1],
        ).start()

    for_slots(tm, load_ids)

    def drain_ids(ref, sem):
        for units in range(low, low + 2 * skew + 1):
            @pl.when(count_of(tm) == units)
            def _():
                drain(ref.at[pl.ds(0, units * PART)], sem)

    def exchange(peers):
        for slot in range(len(slots)):
            for peer in peers:
                at, units, need = slots[slot]

                def ship(peer=peer, slot=slot, at=at, units=units):
                    send(
                        staged.at[:, piece(source_of(peer, slot), units, 2)],
                        got.at[core, tm, :, pl.ds(at * 2 * PART, units * 2 * PART)],
                        send_sem, recv_sem.at[core * len(slots) + slot], hub_of(peer, place),
                    )

                if need and isinstance(peer, int):
                    if count_of(peer) >= low + need:
                        ship()
                elif need:
                    pl.when(count_of(peer) >= low + need)(ship)
                else:
                    ship()

    @pl.when(leaf)
    def _():
        drain_ids(ids.at[HUB], load_sem.at[1])

        @pl.when(jnp.logical_or(gate, head))
        def _():
            pl.semaphore_wait(near_ok, 1)

        @pl.when(jnp.logical_not(jnp.logical_or(gate, head)))
        def _():
            pl.semaphore_wait(barrier, snaps)

        drain(staged, stage_sem)

        def ship_ids(slot):
            at, units, _ = slots[slot]
            span = pl.ds(at * PART, units * PART)
            send(ids.at[HUB, span], ids.at[1 - HUB, span], ids_send, ids_recv, hub_of(tm, place))

        for_slots(tm, ship_ids)

        @pl.when(head)
        def _():
            exchange(list(range(1, last)) + [0])
            pl.semaphore_wait(barrier, 1)
            pl.semaphore_signal(
                late_ok, inc=1, device_id=hub_of(tm, place), device_id_type=MESH
            )
            exchange([last])

        @pl.when(jnp.logical_not(head))
        def _():
            exchange(others + [tm])

        @pl.when(gate)
        def _():
            pl.semaphore_wait(barrier, last + CORES * snaps * (places - 1))
            for snap in range(snaps):
                pl.semaphore_signal(
                    far_ok, inc=1, device_id=hub_of(snap, place), device_id_type=MESH
                )

    @pl.when(hub)
    def _():
        def load_own(slot):
            at, units, _ = slots[slot]
            pltpu.make_async_copy(
                vel_ref.at[:, piece(source_of(tm, slot), units, 2)],
                got.at[HUB, tm, :, pl.ds(at * 2 * PART, units * 2 * PART)], load_sem.at[0],
            ).start()

        for_slots(tm, load_own)
        pl.semaphore_wait(barrier, last + jnp.where(gate, 1, 0))

        @pl.when(jnp.logical_or(gate, head))
        def _():
            pl.semaphore_signal(
                near_ok, inc=1, device_id=leaf_of(tm, place), device_id_type=MESH
            )

        drain(staged, stage_sem)

        @pl.when(head)
        def _():
            exchange(list(range(1, last)))

        @pl.when(jnp.logical_not(head))
        def _():
            exchange(others)

        shell = lax.broadcasted_iota(jnp.int32, (SHELLS, LANES), 0)

        def spot(j):
            high, wide = divmod(j % PART, PART // 2)
            half, lane = divmod(wide, 2)
            return high, half, pl.ds(lane * LANES, LANES)

        def one_hot(unit, slot):
            at, units, _ = slots[slot]
            for j in range(at * PART, (at + units) * PART):
                same = shell == jnp.broadcast_to(ids[unit, j : j + 1, :], (SHELLS, LANES))
                mxu, half, lanes = spot(j)
                hot[unit, j // PART, mxu, half * SHELLS : (half + 1) * SHELLS, lanes] = jnp.where(
                    same, 1.0, 0.0
                ).astype(jnp.bfloat16)

        drain_ids(ids.at[HUB], load_sem.at[1])
        for_slots(tm, functools.partial(one_hot, HUB))

        @pl.when(head)
        def _():
            pl.semaphore_wait(late_ok, 1)
            exchange([last])

        drain_ids(ids.at[1 - HUB], ids_recv)
        for_slots(tm, functools.partial(one_hot, 1 - HUB))
        for units in range(low, low + 2 * skew + 1):
            @pl.when(count_of(tm) == units)
            def _():
                drain(got.at[HUB, 0, :, pl.ds(0, units * 2 * PART)], load_sem.at[0])

        def prepare(unit, at, row):
            span = pl.ds(at * 2 * PART, 2 * PART)
            real, imag = {}, {}
            for t in range(snaps):
                for c in range(3):
                    split[row, t * 3 + c] = got[unit, t, c, span, :].astype(jnp.float32)
            for t in range(snaps):
                for c in range(3):
                    real[t, c] = split[row, t * 3 + c, pl.ds(0, PART, stride=2), :]
                    imag[t, c] = split[row, t * 3 + c, pl.ds(1, PART, stride=2), :]
            for t in range(snaps):
                for r in range(t, snaps):
                    value = real[t, 0] * real[r, 0] + imag[t, 0] * imag[r, 0]
                    for c in (1, 2):
                        value = value + real[t, c] * real[r, c]
                        value = value + imag[t, c] * imag[r, c]
                    terms[row, (t * snaps + r) * PART : (t * snaps + r + 1) * PART] = value
                    if r > t:
                        value = imag[t, 0] * real[r, 0] - real[t, 0] * imag[r, 0]
                        for c in (1, 2):
                            value = value + imag[t, c] * real[r, c]
                            value = value - real[t, c] * imag[r, c]
                        terms[row, (r * snaps + t) * PART : (r * snaps + t + 1) * PART] = value
            for j in range(PART):
                block = terms[row, pl.ds(j, pairs, stride=PART), :]
                mxu, half, lanes = spot(j)
                lhs[row, mxu, half * pairs : (half + 1) * pairs, lanes] = block.astype(jnp.bfloat16)

        def reduce(count, *sums):
            jobs = []
            for slot, (at, units, need) in enumerate(slots):
                if low + need <= count:
                    for unit in (HUB, 1 - HUB):
                        for step in range(units):
                            jobs.append((unit, slot, at + step, step == 0))

            def stage(n):
                unit, _, at, _ = jobs[n]
                for mxu in range(2):
                    pltpu.matmul_push_rhs(hot[unit, at, mxu], n % 2, mxu, transpose=True)

            stage(0)
            for n, (unit, slot, at, fresh) in enumerate(jobs):
                if fresh:
                    first, units, _ = slots[slot]
                    senders = snaps - 1 if unit == HUB else snaps
                    span = pl.ds(first * 2 * PART, units * 2 * PART)
                    drain(
                        got.at[unit, pl.ds(0, senders), :, span], recv_sem.at[unit * len(slots) + slot]
                    )
                if n + 1 < len(jobs):
                    stage(n + 1)
                prepare(unit, at, n % 2)
                for mxu in range(2):
                    pltpu.matmul_acc_lhs(sums[mxu], lhs[n % 2, mxu], load_staged_rhs=n % 2)

        def multiply(*sums):
            for mxu in range(2):
                pltpu.matmul_pop(sums[mxu])
            for units in range(low, low + 2 * skew + 1):
                pl.when(count_of(tm) == units)(functools.partial(reduce, units, *sums))
            value = None
            for mxu in range(2):
                both = pltpu.matmul_pop(sums[mxu])
                both = both[:pairs, :SHELLS] + both[pairs:, SHELLS:]
                value = both if value is None else value + both
            mine[...] = value

        pl.run_scoped(multiply, *(pltpu.ACC(mxu)((2 * pairs, 2 * SHELLS), jnp.float32) for mxu in range(2)))

        diagonal = mine[pl.ds(0, snaps, stride=snaps + 1), :]
        for t in range(snaps):
            packs[t, :snaps] = mine[pl.ds(t * snaps, snaps), :]
            packs[t, snaps : 2 * snaps] = mine[pl.ds(t, snaps, stride=snaps), :]
            packs[t, 2 * snaps :] = diagonal
        pl.semaphore_wait(far_ok, 1)
        for where in range(places):
            for snap in range(snaps):
                send(packs.at[snap], inbox.at[me], pack_send, pack_recv, leaf_of(snap, where))

                @pl.when(me != where * snaps + snap)
                def _():
                    send(packs.at[snap], inbox.at[me], pack_send, pack_recv, hub_of(snap, where))
        inbox[me] = packs[tm]
        drain(inbox.at[pl.ds(0, snaps * places - 1)], pack_recv)

    @pl.when(leaf)
    def _():
        drain(inbox.at[pl.ds(0, snaps * places)], pack_recv)

    value = inbox[0]
    for n in range(1, snaps * places):
        value = value + inbox[n]
    total[...] = value

    load_order.wait()
    across = total[:snaps]
    down = total[snaps : 2 * snaps]
    spectra = total[2 * snaps :]
    own_spectrum = total[pl.ds(2 * snaps + tm, 1), :]
    which = lax.broadcasted_iota(jnp.int32, (snaps, SHELLS), 0)
    down = jnp.where(which == tm, 0.0, down)
    ready[...] = (across * across + down * down) / (own_spectrum * spectra)
    for j in range(snaps):
        coh_ref[0, j : j + 1, :] = ready[pl.ds(order[j], 1), :]
    spec_ref[...] = own_spectrum

    @pl.when(leaf)
    def _():
        drain(staged, send_sem)
        drain_ids(ids.at[HUB], ids_send)

    @pl.when(hub)
    def _():
        for units in range(low, low + 2 * skew + 1):
            @pl.when(count_of(tm) == units)
            def _():
                drain(staged.at[:, pl.ds(0, 2 * (blocks - units * PART))], send_sem)
        drain(inbox.at[pl.ds(0, 2 * snaps * places - 1)], pack_send)


def put(coh_ref, spec_ref, coh_out, spec_out, sems):
    copies = [
        pltpu.make_async_copy(coh_ref, coh_out, sems.at[0]),
        pltpu.make_async_copy(spec_ref, spec_out, sems.at[1]),
    ]
    for copy in copies:
        copy.start()
    for copy in copies:
        copy.wait()


def body(velocity, shell_index, ref_order):
    snaps = lax.axis_size("tm")
    slabs = lax.axis_size("slab")
    places = slabs // CORES
    modes = velocity.shape[3]
    blocks = modes // LANES
    rows = blocks // snaps
    _, skew, low, slots = plan(rows)
    most = slots[-1][0] + 1
    pairs = snaps * snaps
    high = 3 * snaps
    vel = velocity.reshape(3, 2, blocks, LANES).transpose(0, 2, 1, 3)
    vel = vel.reshape(3, 2 * blocks, LANES)
    ids = shell_index.reshape(blocks, LANES)
    coherence, spectrum = pl.pallas_call(
        functools.partial(kernel, snaps, slabs, rows),
        out_shape=(
            pltpu.VMEM((1, snaps, SHELLS), jnp.float32),
            pltpu.VMEM((1, SHELLS), jnp.float32),
        ),
        in_specs=[
            pl.BlockSpec(memory_space=pl.ANY),
            pl.BlockSpec(memory_space=pl.ANY),
            pl.BlockSpec(memory_space=pl.ANY),
        ],
        out_specs=(
            pl.BlockSpec(memory_space=pltpu.VMEM),
            pl.BlockSpec(memory_space=pltpu.VMEM),
        ),
        scratch_shapes=[
            pltpu.VMEM((3, 2 * blocks, LANES), jnp.bfloat16),
            pltpu.VMEM((CORES, most * PART, LANES), jnp.int32),
            pltpu.SMEM((snaps,), jnp.int32),
            pltpu.VMEM((CORES, snaps, 3, most * 2 * PART, LANES), jnp.bfloat16),
            pltpu.VMEM((2, snaps * 3, 2 * PART, LANES), jnp.float32),
            pltpu.VMEM((2, pairs * PART, LANES), jnp.float32),
            pltpu.VMEM((2, 2, 2 * pairs, 2 * LANES), jnp.bfloat16),
            pltpu.VMEM((CORES, most, 2, 2 * SHELLS, 2 * LANES), jnp.bfloat16),
            pltpu.VMEM((pairs, SHELLS), jnp.float32),
            pltpu.VMEM((snaps, high, SHELLS), jnp.float32),
            pltpu.VMEM((2 * snaps * places, high, SHELLS), jnp.float32),
            pltpu.VMEM((high, SHELLS), jnp.float32),
            pltpu.VMEM((snaps, SHELLS), jnp.float32),
            pltpu.SemaphoreType.DMA((3,)),
            pltpu.SemaphoreType.DMA,
            pltpu.SemaphoreType.DMA,
            pltpu.SemaphoreType.DMA,
            pltpu.SemaphoreType.DMA,
            pltpu.SemaphoreType.DMA((CORES * len(slots),)),
            pltpu.SemaphoreType.DMA,
            pltpu.SemaphoreType.DMA,
            pltpu.SemaphoreType.REGULAR,
            pltpu.SemaphoreType.REGULAR,
            pltpu.SemaphoreType.REGULAR,
        ],
        compiler_params=pltpu.CompilerParams(collective_id=0, has_side_effects=True),
    )(vel, ids, ref_order)
    coherence = pltpu.with_memory_space_constraint(coherence, pltpu.VMEM)
    spectrum = pltpu.with_memory_space_constraint(spectrum, pltpu.VMEM)
    return pl.pallas_call(
        put,
        out_shape=(
            jax.ShapeDtypeStruct((1, snaps, SHELLS), jnp.float32),
            jax.ShapeDtypeStruct((1, SHELLS), jnp.float32),
        ),
        in_specs=[pl.BlockSpec(memory_space=pltpu.VMEM)] * 2,
        out_specs=(pl.BlockSpec(memory_space=pl.ANY),) * 2,
        scratch_shapes=[pltpu.SemaphoreType.DMA((2,))],
    )(coherence, spectrum)


def solution(mesh):
    in_specs = (P("tm", None, None, "slab"), P("slab"), P())
    out_specs = (P("tm", None, None), P("tm", None))
    return jax.shard_map(body, mesh=mesh, in_specs=in_specs, out_specs=out_specs, check_vma=False)
```

```python
import functools

import jax
import jax.numpy as jnp
from jax import lax
from jax.experimental import pallas as pl
from jax.experimental.pallas import tpu as pltpu
from jax.sharding import PartitionSpec as P

SHELLS = 128
LANES = 128
CORES = 2
HUB = 1
PART = 8
MESH = pl.DeviceIdType.MESH


def plan(rows):
    base = rows // PART
    skew = 1 if base >= 3 else 0
    low = base - skew
    slots = [(0, low - 1, 0)] if low > 1 else []
    slots += [(low - 1 + extra, 1, extra) for extra in range(2 * skew + 1)]
    return base, skew, low, slots


def kernel(
    snaps, slabs, rows,
    vel_ref, ids_ref, order_ref,
    coh_ref, spec_ref,
    staged, ids, order, got, split, terms, lhs, hot, mine, packs, inbox, total, ready,
    load_sem, stage_sem, ids_recv, send_sem, recv_sem, pack_recv,
    near_ok, far_ok,
):
    tm = lax.axis_index("tm")
    slab = lax.axis_index("slab")
    core = lax.rem(slab, CORES)
    place = lax.div(slab, CORES)
    places = slabs // CORES
    pairs = snaps * snaps
    blocks = rows * snaps
    base, skew, low, slots = plan(rows)
    counts = range(low, low + 2 * skew + 1)
    hub = core == HUB
    leaf = core != HUB
    me = place * snaps + tm
    last = snaps - 1
    gate = tm == last
    head = tm == 0

    others = []
    for high in reversed(range(snaps // 2)):
        for low_bit in (1, 0):
            other_high = lax.rem(lax.div(tm, 2) + high, snaps // 2)
            others.append(other_high * 2 + lax.rem(lax.rem(tm, 2) + low_bit, 2))
    others = others[:-1]
    aways = [lax.rem(place + offset, places) for offset in range(1, places)]

    def hub_of(snap, where):
        return (snap, where * CORES + HUB)

    def leaf_of(snap, where):
        return (snap, where * CORES + 1 - HUB)

    def count_of(snap):
        if isinstance(snap, int):
            return base + (skew if snap == 0 else 0) - (skew if snap == last else 0)
        return base + jnp.where(snap == 0, skew, 0) - jnp.where(snap == last, skew, 0)

    def source_of(snap, slot):
        first = snap * base
        if skew:
            first = first + (jnp.where(snap == 0, 0, skew) if not isinstance(snap, int) else (skew if snap else 0))
        return first + slots[slot][0]

    def piece(start, units, scale):
        size = PART * scale
        if isinstance(start, int):
            return pl.ds(start * size, units * size)
        return pl.ds(pl.multiple_of(start * size, size), units * size)

    barrier = pltpu.get_barrier_semaphore()

    def tell(device):
        pl.semaphore_signal(barrier, inc=1, device_id=device, device_id_type=MESH)

    def send(src, dst, send_to, recv_at, device):
        pltpu.make_async_remote_copy(
            src_ref=src, dst_ref=dst, send_sem=send_to, recv_sem=recv_at,
            device_id=device, device_id_type=MESH,
        ).start()

    def drain(ref, sem):
        pltpu.make_async_copy(ref, ref, sem).wait()

    def for_slots(snap, run):
        for slot, (_, _, need) in enumerate(slots):
            if need:
                pl.when(count_of(snap) >= low + need)(functools.partial(run, slot))
            else:
                run(slot)

    load_order = pltpu.make_async_copy(order_ref, order, load_sem.at[1])
    lead = slots[0][1]
    spans = [
        [piece(source_of(snap, 0), lead, 2) for snap in range(snaps)],
        [
            piece(source_of(snap, 0) + lead, count_of(snap) - lead, 2)
            for snap in range(snaps) if count_of(snap) > lead
        ],
    ]
    for n, some in enumerate(spans):
        for span in some:
            pltpu.make_async_copy(vel_ref.at[:, span], staged.at[:, span], stage_sem).start()

    @pl.when(leaf)
    def _():
        @pl.when(gate)
        def _():
            tell(hub_of(tm, place))

        @pl.when(jnp.logical_not(gate))
        def _():
            tell(leaf_of(last, place))

        @pl.when(head)
        def _():
            tell(hub_of(tm, place))

    @pl.when(hub)
    def _():
        @pl.when(gate)
        def _():
            tell(leaf_of(0, place))
            for snap in range(1, last):
                tell(hub_of(snap, place))

        @pl.when(jnp.logical_not(gate))
        def _():
            for snap in range(snaps):
                @pl.when(tm != snap)
                def _():
                    tell(hub_of(snap, place))

        for snap in range(1, last):
            tell(leaf_of(snap, place))

    for away in aways:
        tell(leaf_of(last, away))

    load_order.start()

    def load_ids(slot):
        at, units, _ = slots[slot]
        pltpu.make_async_copy(
            ids_ref.at[piece(source_of(tm, slot), units, 1)],
            ids.at[HUB, pl.ds(at * PART, units * PART)], load_sem.at[0],
        ).start()

    for_slots(tm, load_ids)

    def drain_ids(ref, sem):
        for units in counts:
            @pl.when(count_of(tm) == units)
            def _():
                drain(ref.at[pl.ds(0, units * PART)], sem)

    every = range(len(slots))

    def bell(unit, slot):
        rest = len(slots) + min(slot, 1)
        if isinstance(unit, int):
            return rest if unit == HUB else slot
        return jnp.where(unit == HUB, rest, slot)


    def exchange(peers, waits=False, chosen=every):
        for slot in chosen:
            if waits and slot == 0:
                drain(staged, stage_sem)
            for peer in peers:
                at, units, need = slots[slot]

                def ship(peer=peer, slot=slot, at=at, units=units):
                    send(
                        staged.at[:, piece(source_of(peer, slot), units, 2)],
                        got.at[core, tm, :, pl.ds(at * 2 * PART, units * 2 * PART)],
                        send_sem, recv_sem.at[bell(core, slot)], hub_of(peer, place),
                    )

                if need and isinstance(peer, int):
                    if count_of(peer) >= low + need:
                        ship()
                elif need:
                    pl.when(count_of(peer) >= low + need)(ship)
                else:
                    ship()

    @pl.when(leaf)
    def _():
        drain_ids(ids.at[HUB], load_sem.at[0])

        @pl.when(jnp.logical_or(gate, head))
        def _():
            pl.semaphore_wait(near_ok, 1)

        @pl.when(jnp.logical_not(jnp.logical_or(gate, head)))
        def _():
            pl.semaphore_wait(barrier, snaps)

        def ship_ids(slot):
            at, units, _ = slots[slot]
            span = pl.ds(at * PART, units * PART)
            send(ids.at[HUB, span], ids.at[1 - HUB, span], send_sem, ids_recv, hub_of(tm, place))

        for_slots(tm, ship_ids)

        @pl.when(head)
        def _():
            exchange(list(range(1, last)) + [0], True)
            pl.semaphore_wait(barrier, 1)
            pl.semaphore_signal(
                near_ok, inc=1, device_id=hub_of(tm, place), device_id_type=MESH
            )
            exchange([last])

        @pl.when(jnp.logical_not(head))
        def _():
            exchange(others + [tm], True)

        @pl.when(gate)
        def _():
            pl.semaphore_wait(barrier, last + CORES * snaps * (places - 1))
            for snap in range(snaps):
                pl.semaphore_signal(
                    far_ok, inc=1, device_id=hub_of(snap, place), device_id_type=MESH
                )

    @pl.when(hub)
    def _():
        def load_own(slot):
            at, units, _ = slots[slot]
            pltpu.make_async_copy(
                vel_ref.at[:, piece(source_of(tm, slot), units, 2)],
                got.at[HUB, tm, :, pl.ds(at * 2 * PART, units * 2 * PART)], load_sem.at[0],
            ).start()

        for_slots(tm, load_own)
        pl.semaphore_wait(barrier, last + jnp.where(gate, 1, 0))

        @pl.when(jnp.logical_or(gate, head))
        def _():
            pl.semaphore_signal(
                near_ok, inc=1, device_id=leaf_of(tm, place), device_id_type=MESH
            )

        @pl.when(head)
        def _():
            exchange(list(range(1, last)), True, every[:1])

        @pl.when(jnp.logical_not(head))
        def _():
            exchange(others, True, every[:1])

        shell = lax.broadcasted_iota(jnp.int32, (SHELLS, LANES), 0)

        def spot(j):
            high, wide = divmod(j % PART, PART // 2)
            half, lane = divmod(wide, 2)
            return high, half, pl.ds(lane * LANES, LANES)

        def one_hot(unit, slot):
            at, units, _ = slots[slot]
            for j in range(at * PART, (at + units) * PART):
                same = shell == jnp.broadcast_to(ids[unit, j : j + 1, :], (SHELLS, LANES))
                mxu, half, lanes = spot(j)
                hot[unit, j // PART, mxu, half * SHELLS : (half + 1) * SHELLS, lanes] = jnp.where(
                    same, 1.0, 0.0
                ).astype(jnp.bfloat16)

        for units in counts:
            @pl.when(count_of(tm) == units)
            def _():
                drain(hot.at[0, pl.ds(0, units), 0, pl.ds(0, 4 * PART)], load_sem.at[0])

        for_slots(tm, functools.partial(one_hot, HUB))

        @pl.when(head)
        def _():
            exchange(list(range(1, last)), True, every[1:])
            pl.semaphore_wait(near_ok, 1)
            exchange([last])

        @pl.when(jnp.logical_not(head))
        def _():
            exchange(others, True, every[1:])

        drain_ids(ids.at[1 - HUB], ids_recv)
        for_slots(tm, functools.partial(one_hot, 1 - HUB))
        def prepare(unit, at, row):
            span = pl.ds(at * 2 * PART, 2 * PART)
            real, imag = {}, {}
            for t in range(snaps):
                for c in range(3):
                    split[row, t * 3 + c] = got[unit, t, c, span, :].astype(jnp.float32)
            for t in range(snaps):
                for c in range(3):
                    real[t, c] = split[row, t * 3 + c, pl.ds(0, PART, stride=2), :]
                    imag[t, c] = split[row, t * 3 + c, pl.ds(1, PART, stride=2), :]
            for t in range(snaps):
                for r in range(t, snaps):
                    value = real[t, 0] * real[r, 0] + imag[t, 0] * imag[r, 0]
                    for c in (1, 2):
                        value = value + real[t, c] * real[r, c]
                        value = value + imag[t, c] * imag[r, c]
                    terms[row, (t * snaps + r) * PART : (t * snaps + r + 1) * PART] = value
                    if r > t:
                        value = imag[t, 0] * real[r, 0] - real[t, 0] * imag[r, 0]
                        for c in (1, 2):
                            value = value + imag[t, c] * real[r, c]
                            value = value - real[t, c] * imag[r, c]
                        terms[row, (r * snaps + t) * PART : (r * snaps + t + 1) * PART] = value
            for j in range(PART):
                block = terms[row, pl.ds(j, pairs, stride=PART), :]
                mxu, half, lanes = spot(j)
                lhs[row, mxu, half * pairs : (half + 1) * pairs, lanes] = block.astype(jnp.bfloat16)

        def reduce(count, *sums):
            live = [n for n, (_, _, need) in enumerate(slots) if low + need <= count]
            groups = [(HUB, live[:1])] + [(1 - HUB, [n]) for n in live]
            if live[1:]:
                groups.insert(len(groups) - 1, (HUB, live[1:]))
            jobs = []
            for unit, some in groups:
                spots = [slots[n][0] + step for n in some for step in range(slots[n][1])]
                jobs += [(unit, some[0], at, len(spots) if at == spots[0] else 0) for at in spots]

            def stage(n):
                unit, _, at, _ = jobs[n]
                for mxu in range(2):
                    pltpu.matmul_push_rhs(hot[unit, at, mxu], n % 2, mxu, transpose=True)

            stage(0)
            for n, (unit, slot, at, fresh) in enumerate(jobs):
                if fresh:
                    senders = snaps - 1 if unit == HUB else snaps
                    span = pl.ds(at * 2 * PART, fresh * 2 * PART)
                    drain(got.at[unit, pl.ds(0, senders), :, span], recv_sem.at[bell(unit, slot)])
                if n + 1 < len(jobs):
                    stage(n + 1)
                prepare(unit, at, n % 2)
                for mxu in range(2):
                    pltpu.matmul_acc_lhs(sums[mxu], lhs[n % 2, mxu], load_staged_rhs=n % 2)

        def multiply(*sums):
            for mxu in range(2):
                pltpu.matmul_pop(sums[mxu])
            for units in counts:
                pl.when(count_of(tm) == units)(functools.partial(reduce, units, *sums))
            value = None
            for mxu in range(2):
                both = pltpu.matmul_pop(sums[mxu])
                both = both[:pairs, :SHELLS] + both[pairs:, SHELLS:]
                value = both if value is None else value + both
            mine[...] = value

        pl.run_scoped(multiply, *(pltpu.ACC(mxu)((2 * pairs, 2 * SHELLS), jnp.float32) for mxu in range(2)))

        diagonal = mine[pl.ds(0, snaps, stride=snaps + 1), :]
        for t in range(snaps):
            packs[t, :snaps] = mine[pl.ds(t * snaps, snaps), :]
            packs[t, snaps : 2 * snaps] = mine[pl.ds(t, snaps, stride=snaps), :]
            packs[t, 2 * snaps :] = diagonal
        pl.semaphore_wait(far_ok, 1)
        for where in range(places):
            for snap in range(snaps):
                send(packs.at[snap], inbox.at[me], send_sem, pack_recv, leaf_of(snap, where))

                @pl.when(me != where * snaps + snap)
                def _():
                    send(packs.at[snap], inbox.at[me], send_sem, pack_recv, hub_of(snap, where))
        inbox[me] = packs[tm]
        drain(inbox.at[pl.ds(0, snaps * places - 1)], pack_recv)

    @pl.when(leaf)
    def _():
        drain(inbox.at[pl.ds(0, snaps * places)], pack_recv)

    value = inbox[0]
    for n in range(1, snaps * places):
        value = value + inbox[n]
    total[...] = value

    load_order.wait()
    across = total[:snaps]
    down = total[snaps : 2 * snaps]
    spectra = total[2 * snaps :]
    own_spectrum = total[pl.ds(2 * snaps + tm, 1), :]
    which = lax.broadcasted_iota(jnp.int32, (snaps, SHELLS), 0)
    down = jnp.where(which == tm, 0.0, down)
    ready[...] = (across * across + down * down) / (own_spectrum * spectra)
    for j in range(snaps):
        coh_ref[0, j : j + 1, :] = ready[pl.ds(order[j], 1), :]
    spec_ref[...] = own_spectrum

    @pl.when(leaf)
    def _():
        drain(staged, send_sem)
        drain_ids(ids.at[HUB], send_sem)

    @pl.when(hub)
    def _():
        for units in counts:
            @pl.when(count_of(tm) == units)
            def _():
                drain(staged.at[:, pl.ds(0, 2 * (blocks - units * PART))], send_sem)
        drain(inbox.at[pl.ds(0, 2 * snaps * places - 1)], send_sem)


def put(coh_ref, spec_ref, coh_out, spec_out, sems):
    copies = [
        pltpu.make_async_copy(coh_ref, coh_out, sems.at[0]),
        pltpu.make_async_copy(spec_ref, spec_out, sems.at[1]),
    ]
    for copy in copies:
        copy.start()
    for copy in copies:
        copy.wait()


def body(velocity, shell_index, ref_order):
    snaps = lax.axis_size("tm")
    slabs = lax.axis_size("slab")
    places = slabs // CORES
    modes = velocity.shape[3]
    blocks = modes // LANES
    rows = blocks // snaps
    _, skew, low, slots = plan(rows)
    most = slots[-1][0] + 1
    pairs = snaps * snaps
    high = 3 * snaps
    vel = velocity.reshape(3, 2, blocks, LANES).transpose(0, 2, 1, 3)
    vel = vel.reshape(3, 2 * blocks, LANES)
    ids = shell_index.reshape(blocks, LANES)
    coherence, spectrum = pl.pallas_call(
        functools.partial(kernel, snaps, slabs, rows),
        out_shape=(
            pltpu.VMEM((1, snaps, SHELLS), jnp.float32),
            pltpu.VMEM((1, SHELLS), jnp.float32),
        ),
        in_specs=[
            pl.BlockSpec(memory_space=pl.ANY),
            pl.BlockSpec(memory_space=pl.ANY),
            pl.BlockSpec(memory_space=pl.ANY),
        ],
        out_specs=(
            pl.BlockSpec(memory_space=pltpu.VMEM),
            pl.BlockSpec(memory_space=pltpu.VMEM),
        ),
        scratch_shapes=[
            pltpu.VMEM((3, 2 * blocks, LANES), jnp.bfloat16),
            pltpu.VMEM((CORES, most * PART, LANES), jnp.int32),
            pltpu.SMEM((snaps,), jnp.int32),
            pltpu.VMEM((CORES, snaps, 3, most * 2 * PART, LANES), jnp.bfloat16),
            pltpu.VMEM((2, snaps * 3, 2 * PART, LANES), jnp.float32),
            pltpu.VMEM((2, pairs * PART, LANES), jnp.float32),
            pltpu.VMEM((2, 2, 2 * pairs, 2 * LANES), jnp.bfloat16),
            pltpu.VMEM((CORES, most, 2, 2 * SHELLS, 2 * LANES), jnp.bfloat16),
            pltpu.VMEM((pairs, SHELLS), jnp.float32),
            pltpu.VMEM((snaps, high, SHELLS), jnp.float32),
            pltpu.VMEM((2 * snaps * places, high, SHELLS), jnp.float32),
            pltpu.VMEM((high, SHELLS), jnp.float32),
            pltpu.VMEM((snaps, SHELLS), jnp.float32),
            pltpu.SemaphoreType.DMA((2,)),
            pltpu.SemaphoreType.DMA,
            pltpu.SemaphoreType.DMA,
            pltpu.SemaphoreType.DMA,
            pltpu.SemaphoreType.DMA((len(slots) + 2,)),
            pltpu.SemaphoreType.DMA,
            pltpu.SemaphoreType.REGULAR,
            pltpu.SemaphoreType.REGULAR,
        ],
        compiler_params=pltpu.CompilerParams(collective_id=0, has_side_effects=True),
    )(vel, ids, ref_order)
    coherence = pltpu.with_memory_space_constraint(coherence, pltpu.VMEM)
    spectrum = pltpu.with_memory_space_constraint(spectrum, pltpu.VMEM)
    return pl.pallas_call(
        put,
        out_shape=(
            jax.ShapeDtypeStruct((1, snaps, SHELLS), jnp.float32),
            jax.ShapeDtypeStruct((1, SHELLS), jnp.float32),
        ),
        in_specs=[pl.BlockSpec(memory_space=pltpu.VMEM)] * 2,
        out_specs=(pl.BlockSpec(memory_space=pl.ANY),) * 2,
        scratch_shapes=[pltpu.SemaphoreType.DMA((2,))],
    )(coherence, spectrum)


def solution(mesh):
    in_specs = (P("tm", None, None, "slab"), P("slab"), P())
    out_specs = (P("tm", None, None), P("tm", None))
    return jax.shard_map(body, mesh=mesh, in_specs=in_specs, out_specs=out_specs, check_vma=False)
```

```python
import functools

import jax
import jax.numpy as jnp
from jax import lax
from jax.experimental import pallas as pl
from jax.experimental.pallas import tpu as pltpu
from jax.sharding import PartitionSpec as P

SHELLS = 128
LANES = 128
CORES = 2
HUB = 1
PART = 8
MESH = pl.DeviceIdType.MESH


def plan(rows):
    base = rows // PART
    skew = 1 if base >= 3 else 0
    low = base - skew
    slots = [(0, low - 1, 0)] if low > 1 else []
    slots += [(low - 1 + extra, 1, extra) for extra in range(2 * skew + 1)]
    return base, skew, low, slots


def kernel(
    snaps, slabs, rows,
    vel_ref, ids_ref, order_ref,
    coh_ref, spec_ref,
    staged, ids, order, got, split, terms, lhs, hot, mine, packs, inbox, total, ready,
    load_sem, stage_sem, ids_recv, send_sem, recv_sem, pack_recv,
    near_ok, far_ok,
):
    tm = lax.axis_index("tm")
    slab = lax.axis_index("slab")
    core = lax.rem(slab, CORES)
    place = lax.div(slab, CORES)
    places = slabs // CORES
    pairs = snaps * snaps
    blocks = rows * snaps
    base, skew, low, slots = plan(rows)
    counts = range(low, low + 2 * skew + 1)
    hub = core == HUB
    leaf = core != HUB
    me = place * snaps + tm
    last = snaps - 1
    gate = tm == last
    head = tm == 0

    others = []
    for high in reversed(range(snaps // 2)):
        for low_bit in (1, 0):
            other_high = lax.rem(lax.div(tm, 2) + high, snaps // 2)
            others.append(other_high * 2 + lax.rem(lax.rem(tm, 2) + low_bit, 2))
    others = others[:-1]
    aways = [lax.rem(place + offset, places) for offset in range(1, places)]

    def hub_of(snap, where):
        return (snap, where * CORES + HUB)

    def leaf_of(snap, where):
        return (snap, where * CORES + 1 - HUB)

    def count_of(snap):
        if isinstance(snap, int):
            return base + (skew if snap == 0 else 0) - (skew if snap == last else 0)
        return base + jnp.where(snap == 0, skew, 0) - jnp.where(snap == last, skew, 0)

    def source_of(snap, slot):
        first = snap * base
        if skew:
            first = first + (jnp.where(snap == 0, 0, skew) if not isinstance(snap, int) else (skew if snap else 0))
        return first + slots[slot][0]

    def piece(start, units, scale):
        size = PART * scale
        if isinstance(start, int):
            return pl.ds(start * size, units * size)
        return pl.ds(pl.multiple_of(start * size, size), units * size)

    barrier = pltpu.get_barrier_semaphore()

    def tell(device):
        pl.semaphore_signal(barrier, inc=1, device_id=device, device_id_type=MESH)

    def send(src, dst, send_to, recv_at, device):
        pltpu.make_async_remote_copy(
            src_ref=src, dst_ref=dst, send_sem=send_to, recv_sem=recv_at,
            device_id=device, device_id_type=MESH,
        ).start()

    def drain(ref, sem):
        pltpu.make_async_copy(ref, ref, sem).wait()

    def for_slots(snap, run):
        for slot, (_, _, need) in enumerate(slots):
            if need:
                pl.when(count_of(snap) >= low + need)(functools.partial(run, slot))
            else:
                run(slot)

    load_order = pltpu.make_async_copy(order_ref, order, load_sem.at[1])
    for part in range(snaps):
        span = pl.ds(part * 2 * rows, 2 * rows)
        pltpu.make_async_copy(vel_ref.at[:, span], staged.at[:, span], stage_sem).start()

    @pl.when(leaf)
    def _():
        @pl.when(gate)
        def _():
            tell(hub_of(tm, place))

        @pl.when(jnp.logical_not(gate))
        def _():
            tell(leaf_of(last, place))

        @pl.when(head)
        def _():
            tell(hub_of(tm, place))

    @pl.when(hub)
    def _():
        @pl.when(gate)
        def _():
            tell(leaf_of(0, place))
            for snap in range(1, last):
                tell(hub_of(snap, place))

        @pl.when(jnp.logical_not(gate))
        def _():
            for snap in range(snaps):
                @pl.when(tm != snap)
                def _():
                    tell(hub_of(snap, place))

        for snap in range(1, last):
            tell(leaf_of(snap, place))

    for away in aways:
        tell(leaf_of(last, away))

    load_order.start()

    def load_ids(slot):
        at, units, _ = slots[slot]
        pltpu.make_async_copy(
            ids_ref.at[piece(source_of(tm, slot), units, 1)],
            ids.at[HUB, pl.ds(at * PART, units * PART)], load_sem.at[0],
        ).start()

    for_slots(tm, load_ids)

    def drain_ids(ref, sem):
        for units in counts:
            @pl.when(count_of(tm) == units)
            def _():
                drain(ref.at[pl.ds(0, units * PART)], sem)

    every = range(len(slots))

    def bell(unit, slot):
        rest = len(slots) + min(slot, 1)
        if isinstance(unit, int):
            return rest if unit == HUB else slot
        return jnp.where(unit == HUB, rest, slot)


    def exchange(peers, waits=False, chosen=every):
        for slot in chosen:
            if waits and slot == 0:
                drain(staged, stage_sem)
            for peer in peers:
                at, units, need = slots[slot]

                def ship(peer=peer, slot=slot, at=at, units=units):
                    send(
                        staged.at[:, piece(source_of(peer, slot), units, 2)],
                        got.at[core, tm, :, pl.ds(at * 2 * PART, units * 2 * PART)],
                        send_sem, recv_sem.at[bell(core, slot)], hub_of(peer, place),
                    )

                if need and isinstance(peer, int):
                    if count_of(peer) >= low + need:
                        ship()
                elif need:
                    pl.when(count_of(peer) >= low + need)(ship)
                else:
                    ship()

    @pl.when(leaf)
    def _():
        drain_ids(ids.at[HUB], load_sem.at[0])

        @pl.when(jnp.logical_or(gate, head))
        def _():
            pl.semaphore_wait(near_ok, 1)

        @pl.when(jnp.logical_not(jnp.logical_or(gate, head)))
        def _():
            pl.semaphore_wait(barrier, snaps)

        def ship_ids(slot):
            at, units, _ = slots[slot]
            span = pl.ds(at * PART, units * PART)
            send(ids.at[HUB, span], ids.at[1 - HUB, span], send_sem, ids_recv, hub_of(tm, place))

        for_slots(tm, ship_ids)

        @pl.when(head)
        def _():
            exchange(list(range(1, last)) + [0], True)
            pl.semaphore_wait(barrier, 1)
            pl.semaphore_signal(
                near_ok, inc=1, device_id=hub_of(tm, place), device_id_type=MESH
            )
            exchange([last])

        @pl.when(jnp.logical_not(head))
        def _():
            exchange(others + [tm], True)

        @pl.when(gate)
        def _():
            pl.semaphore_wait(barrier, last + CORES * snaps * (places - 1))
            for snap in range(snaps):
                pl.semaphore_signal(
                    far_ok, inc=1, device_id=hub_of(snap, place), device_id_type=MESH
                )

    @pl.when(hub)
    def _():
        def load_own(slot):
            at, units, _ = slots[slot]
            pltpu.make_async_copy(
                vel_ref.at[:, piece(source_of(tm, slot), units, 2)],
                got.at[HUB, tm, :, pl.ds(at * 2 * PART, units * 2 * PART)], load_sem.at[0],
            ).start()

        for_slots(tm, load_own)
        pl.semaphore_wait(barrier, last + jnp.where(gate, 1, 0))

        @pl.when(jnp.logical_or(gate, head))
        def _():
            pl.semaphore_signal(
                near_ok, inc=1, device_id=leaf_of(tm, place), device_id_type=MESH
            )

        @pl.when(head)
        def _():
            exchange(list(range(1, last)), True, every[:1])

        @pl.when(jnp.logical_not(head))
        def _():
            exchange(others, True, every[:1])

        shell = lax.broadcasted_iota(jnp.int32, (SHELLS, LANES), 0)

        def spot(j):
            high, wide = divmod(j % PART, PART // 2)
            half, lane = divmod(wide, 2)
            return high, half, pl.ds(lane * LANES, LANES)

        def one_hot(unit, slot):
            at, units, _ = slots[slot]
            for j in range(at * PART, (at + units) * PART):
                same = shell == jnp.broadcast_to(ids[unit, j : j + 1, :], (SHELLS, LANES))
                mxu, half, lanes = spot(j)
                hot[unit, j // PART, mxu, half * SHELLS : (half + 1) * SHELLS, lanes] = jnp.where(
                    same, 1.0, 0.0
                ).astype(jnp.bfloat16)

        for units in counts:
            @pl.when(count_of(tm) == units)
            def _():
                drain(hot.at[0, pl.ds(0, units), 0, pl.ds(0, 4 * PART)], load_sem.at[0])

        for_slots(tm, functools.partial(one_hot, HUB))

        @pl.when(head)
        def _():
            exchange(list(range(1, last)), True, every[1:])
            pl.semaphore_wait(near_ok, 1)
            exchange([last])

        @pl.when(jnp.logical_not(head))
        def _():
            exchange(others, True, every[1:])

        drain_ids(ids.at[1 - HUB], ids_recv)
        for_slots(tm, functools.partial(one_hot, 1 - HUB))
        def prepare(unit, at, row):
            span = pl.ds(at * 2 * PART, 2 * PART)
            real, imag = {}, {}
            for t in range(snaps):
                for c in range(3):
                    split[row, t * 3 + c] = got[unit, t, c, span, :].astype(jnp.float32)
            for t in range(snaps):
                for c in range(3):
                    real[t, c] = split[row, t * 3 + c, pl.ds(0, PART, stride=2), :]
                    imag[t, c] = split[row, t * 3 + c, pl.ds(1, PART, stride=2), :]
            for t in range(snaps):
                for r in range(t, snaps):
                    value = real[t, 0] * real[r, 0] + imag[t, 0] * imag[r, 0]
                    for c in (1, 2):
                        value = value + real[t, c] * real[r, c]
                        value = value + imag[t, c] * imag[r, c]
                    terms[row, (t * snaps + r) * PART : (t * snaps + r + 1) * PART] = value
                    if r > t:
                        value = imag[t, 0] * real[r, 0] - real[t, 0] * imag[r, 0]
                        for c in (1, 2):
                            value = value + imag[t, c] * real[r, c]
                            value = value - real[t, c] * imag[r, c]
                        terms[row, (r * snaps + t) * PART : (r * snaps + t + 1) * PART] = value
            for j in range(PART):
                block = terms[row, pl.ds(j, pairs, stride=PART), :]
                mxu, half, lanes = spot(j)
                lhs[row, mxu, half * pairs : (half + 1) * pairs, lanes] = block.astype(jnp.bfloat16)

        def reduce(count, *sums):
            live = [n for n, (_, _, need) in enumerate(slots) if low + need <= count]
            groups = [(HUB, live[:1])] + [(1 - HUB, [n]) for n in live]
            if live[1:]:
                groups.insert(len(groups) - 1, (HUB, live[1:]))
            jobs = []
            for unit, some in groups:
                spots = [slots[n][0] + step for n in some for step in range(slots[n][1])]
                jobs += [(unit, some[0], at, len(spots) if at == spots[0] else 0) for at in spots]

            def stage(n):
                unit, _, at, _ = jobs[n]
                for mxu in range(2):
                    pltpu.matmul_push_rhs(hot[unit, at, mxu], n % 2, mxu, transpose=True)

            stage(0)
            for n, (unit, slot, at, fresh) in enumerate(jobs):
                if fresh:
                    senders = snaps - 1 if unit == HUB else snaps
                    span = pl.ds(at * 2 * PART, fresh * 2 * PART)
                    drain(got.at[unit, pl.ds(0, senders), :, span], recv_sem.at[bell(unit, slot)])
                if n + 1 < len(jobs):
                    stage(n + 1)
                prepare(unit, at, n % 2)
                for mxu in range(2):
                    pltpu.matmul_acc_lhs(sums[mxu], lhs[n % 2, mxu], load_staged_rhs=n % 2)

        def multiply(*sums):
            for mxu in range(2):
                pltpu.matmul_pop(sums[mxu])
            for units in counts:
                pl.when(count_of(tm) == units)(functools.partial(reduce, units, *sums))
            value = None
            for mxu in range(2):
                both = pltpu.matmul_pop(sums[mxu])
                both = both[:pairs, :SHELLS] + both[pairs:, SHELLS:]
                value = both if value is None else value + both
            mine[...] = value

        pl.run_scoped(multiply, *(pltpu.ACC(mxu)((2 * pairs, 2 * SHELLS), jnp.float32) for mxu in range(2)))

        diagonal = mine[pl.ds(0, snaps, stride=snaps + 1), :]
        for t in range(snaps):
            packs[t, :snaps] = mine[pl.ds(t * snaps, snaps), :]
            packs[t, snaps : 2 * snaps] = mine[pl.ds(t, snaps, stride=snaps), :]
            packs[t, 2 * snaps :] = diagonal
        pl.semaphore_wait(far_ok, 1)
        for where in range(places):
            for snap in range(snaps):
                send(packs.at[snap], inbox.at[me], send_sem, pack_recv, leaf_of(snap, where))

                @pl.when(me != where * snaps + snap)
                def _():
                    send(packs.at[snap], inbox.at[me], send_sem, pack_recv, hub_of(snap, where))
        inbox[me] = packs[tm]
        drain(inbox.at[pl.ds(0, snaps * places - 1)], pack_recv)

    @pl.when(leaf)
    def _():
        drain(inbox.at[pl.ds(0, snaps * places)], pack_recv)

    value = inbox[0]
    for n in range(1, snaps * places):
        value = value + inbox[n]
    total[...] = value

    load_order.wait()
    across = total[:snaps]
    down = total[snaps : 2 * snaps]
    spectra = total[2 * snaps :]
    own_spectrum = total[pl.ds(2 * snaps + tm, 1), :]
    which = lax.broadcasted_iota(jnp.int32, (snaps, SHELLS), 0)
    down = jnp.where(which == tm, 0.0, down)
    ready[...] = (across * across + down * down) / (own_spectrum * spectra)
    for j in range(snaps):
        coh_ref[0, j : j + 1, :] = ready[pl.ds(order[j], 1), :]
    spec_ref[...] = own_spectrum

    @pl.when(leaf)
    def _():
        drain(staged, send_sem)
        drain_ids(ids.at[HUB], send_sem)

    @pl.when(hub)
    def _():
        for units in counts:
            @pl.when(count_of(tm) == units)
            def _():
                drain(staged.at[:, pl.ds(0, 2 * (blocks - units * PART))], send_sem)
        drain(inbox.at[pl.ds(0, 2 * snaps * places - 1)], send_sem)


def put(coh_ref, spec_ref, coh_out, spec_out, both, sem):
    pltpu.make_async_copy(coh_ref, coh_out, sem).start()
    pltpu.make_async_copy(spec_ref, spec_out, sem).start()
    pltpu.make_async_copy(both, both, sem).wait()


def body(velocity, shell_index, ref_order):
    snaps = lax.axis_size("tm")
    slabs = lax.axis_size("slab")
    places = slabs // CORES
    modes = velocity.shape[3]
    blocks = modes // LANES
    rows = blocks // snaps
    _, skew, low, slots = plan(rows)
    most = slots[-1][0] + 1
    pairs = snaps * snaps
    high = 3 * snaps
    vel = velocity.reshape(3, 2, blocks, LANES).transpose(0, 2, 1, 3)
    vel = vel.reshape(3, 2 * blocks, LANES)
    ids = shell_index.reshape(blocks, LANES)
    coherence, spectrum = pl.pallas_call(
        functools.partial(kernel, snaps, slabs, rows),
        out_shape=(
            pltpu.VMEM((1, snaps, SHELLS), jnp.float32),
            pltpu.VMEM((1, SHELLS), jnp.float32),
        ),
        in_specs=[
            pl.BlockSpec(memory_space=pl.ANY),
            pl.BlockSpec(memory_space=pl.ANY),
            pl.BlockSpec(memory_space=pl.ANY),
        ],
        out_specs=(
            pl.BlockSpec(memory_space=pltpu.VMEM),
            pl.BlockSpec(memory_space=pltpu.VMEM),
        ),
        scratch_shapes=[
            pltpu.VMEM((3, 2 * blocks, LANES), jnp.bfloat16),
            pltpu.VMEM((CORES, most * PART, LANES), jnp.int32),
            pltpu.SMEM((snaps,), jnp.int32),
            pltpu.VMEM((CORES, snaps, 3, most * 2 * PART, LANES), jnp.bfloat16),
            pltpu.VMEM((2, snaps * 3, 2 * PART, LANES), jnp.float32),
            pltpu.VMEM((2, pairs * PART, LANES), jnp.float32),
            pltpu.VMEM((2, 2, 2 * pairs, 2 * LANES), jnp.bfloat16),
            pltpu.VMEM((CORES, most, 2, 2 * SHELLS, 2 * LANES), jnp.bfloat16),
            pltpu.VMEM((pairs, SHELLS), jnp.float32),
            pltpu.VMEM((snaps, high, SHELLS), jnp.float32),
            pltpu.VMEM((2 * snaps * places, high, SHELLS), jnp.float32),
            pltpu.VMEM((high, SHELLS), jnp.float32),
            pltpu.VMEM((snaps, SHELLS), jnp.float32),
            pltpu.SemaphoreType.DMA((2,)),
            pltpu.SemaphoreType.DMA,
            pltpu.SemaphoreType.DMA,
            pltpu.SemaphoreType.DMA,
            pltpu.SemaphoreType.DMA((len(slots) + 2,)),
            pltpu.SemaphoreType.DMA,
            pltpu.SemaphoreType.REGULAR,
            pltpu.SemaphoreType.REGULAR,
        ],
        compiler_params=pltpu.CompilerParams(collective_id=0, has_side_effects=True),
    )(vel, ids, ref_order)
    coherence = pltpu.with_memory_space_constraint(coherence, pltpu.VMEM)
    spectrum = pltpu.with_memory_space_constraint(spectrum, pltpu.VMEM)
    return pl.pallas_call(
        put,
        out_shape=(
            jax.ShapeDtypeStruct((1, snaps, SHELLS), jnp.float32),
            jax.ShapeDtypeStruct((1, SHELLS), jnp.float32),
        ),
        in_specs=[pl.BlockSpec(memory_space=pltpu.VMEM)] * 2,
        out_specs=(pl.BlockSpec(memory_space=pl.ANY),) * 2,
        scratch_shapes=[pltpu.VMEM((snaps + 1, SHELLS), jnp.float32), pltpu.SemaphoreType.DMA],
    )(coherence, spectrum)


def solution(mesh):
    in_specs = (P("tm", None, None, "slab"), P("slab"), P())
    out_specs = (P("tm", None, None), P("tm", None))
    return jax.shard_map(body, mesh=mesh, in_specs=in_specs, out_specs=out_specs, check_vma=False)
```
